32 devices in a mesh: dp: 32 (over z, y, x, core).
Axes of the slice: x: 2, y: 2, z: 4, core: 2. Of those that a mesh axis runs over, the one named last changes fastest.
Arguments:
- features: bfloat16 [64, 256, 256], P('dp'), may hold values from -6 to 6
- frame_lens: int32 [64], P('dp'), may hold values from 128 to 256
- labels: int32 [64, 48], P('dp'), may hold values from 1 to 255
- label_lens: int32 [64], P('dp'), may hold values from 1 to 48
- w_up: float32 [262144], P('dp'), may hold values from -0.375 to 0.375
- w_down: float32 [262144], P('dp'), may hold values from -0.1875 to 0.1875
- w_out: float32 [65536], P('dp'), may hold values from -1.125 to 1.125
- first_up: float32 [262144], P('dp'), may hold values from -0.00018 to 0.00018
- first_down: float32 [262144], P('dp'), may hold values from -0.00018 to 0.00018
- first_out: float32 [65536], P('dp'), may hold values from -0.00018 to 0.00018
- second_up: float32 [262144], P('dp'), may hold values from 1e-10 to 1e-08
- second_down: float32 [262144], P('dp'), may hold values from 1e-10 to 1e-08
- second_out: float32 [65536], P('dp'), may hold values from 1e-10 to 1e-08
Outputs:
- new_up: float32 [262144], P('dp')
- new_down: float32 [262144], P('dp')
- new_out: float32 [65536], P('dp')
- new_first_up: float32 [262144], P('dp')
- new_first_down: float32 [262144], P('dp')
- new_first_out: float32 [65536], P('dp')
- new_second_up: float32 [262144], P('dp')
- new_second_down: float32 [262144], P('dp')
- new_second_out: float32 [65536], P('dp')
The draws below stay inside these ranges and needn't reach their ends.
Inputs may be any that keep to these rules, and one draw needn't show every extreme that they name: `labels`: 0 is the blank and is not a label.
All inputs are finite; a program needn't handle non-finite values.
Results may differ from the reference program's by a relative error of at most 0.002.
The reference program's roundings to bfloat16 on the way (of `normalized`, `hidden`, `block_out`, `logit_grad`, `ff_grad` and `act_grad`) count: a program that leaves them out, or rounds other values in their place, can miss the bound.
Values may be sent and summed in bfloat16 or wider, within the bound.
A program may use at most 64 MiB of HBM per device.

```python
import math
import jax
import jax.numpy as jnp
from jax import lax

D = 256
FF = 1024
VOCAB = 256
UTT = 2
FRAMES = 256
LABELS = 48
UTTERANCES = 64
N_DP = 32


def set_ends(result, rng, smallest, largest):
    longest = result.shape.index(max(result.shape))
    spots = []
    for shift in (0, 1):
        where = [jax.random.randint(jax.random.fold_in(rng, axis), (), 0, length) for axis, length in enumerate(result.shape)]
        where[longest] = (where[longest] + shift) % result.shape[longest]
        spots.append(tuple(where))
    return result.at[spots[0]].set(smallest).at[spots[1]].set(largest)


def shard_levels(rng, shape, cuts, smallest, top_value):
    def one(axis_at, blocks):
        heights = jax.random.uniform(jax.random.fold_in(jax.random.fold_in(rng, 6), axis_at), (blocks,), jnp.float32, smallest / len(cuts), top_value / len(cuts))
        return jnp.repeat(jnp.exp(heights), shape[axis_at] // blocks).reshape((-1,) + (1,) * (len(shape) - axis_at - 1))

    gain = one(*cuts[0])
    for cut in cuts[1:]:
        gain = gain * one(*cut)
    return gain


def gaussian(own_key, dims, deviation, reach, pieces=(), kind=jnp.bfloat16):
    values = jax.random.normal(own_key, dims, jnp.float32) * deviation
    if len(pieces) > 0:
        values = shard_levels(own_key, dims, pieces, -0.22, 0.18) * values
    return jnp.clip(values, min=-reach, max=reach).astype(kind)


def setup_inputs(seed: int = 0) -> dict:
    key_list = jax.random.split(jax.random.key(seed), 14)
    return {
        "features": gaussian(key_list[0], (UTTERANCES, FRAMES, D), 1.0, 6.0, ((0, 32),)),
        "frame_lens": set_ends(jax.random.randint(key_list[1], (UTTERANCES,), FRAMES // 2, FRAMES + 1), jax.random.fold_in(key_list[1], 1), FRAMES // 2, FRAMES).astype(jnp.int32),
        "labels": set_ends(jax.random.randint(key_list[2], (UTTERANCES, LABELS), 1, VOCAB), jax.random.fold_in(key_list[2], 1), 1, VOCAB - 1).astype(jnp.int32),
        "label_lens": set_ends(jax.random.randint(key_list[3], (UTTERANCES,), 1, LABELS + 1), jax.random.fold_in(key_list[3], 1), 1, LABELS).astype(jnp.int32),
        "w_up": gaussian(key_list[4], (D * FF,), D ** -0.5, 0.375, ((0, 32),), jnp.float32),
        "w_down": gaussian(key_list[5], (FF * D,), FF ** -0.5, 0.1875, ((0, 32),), jnp.float32),
        "w_out": gaussian(key_list[6], (D * VOCAB,), (3.0 / D ** 0.5), 1.125, ((0, 32),), jnp.float32),
        "first_up": gaussian(key_list[7], (D * FF,), (3e-5), 0.00018, ((0, 32),), jnp.float32),
        "first_down": gaussian(key_list[8], (FF * D,), (3e-5), 0.00018, ((0, 32),), jnp.float32),
        "first_out": gaussian(key_list[9], (D * VOCAB,), (3e-5), 0.00018, ((0, 32),), jnp.float32),
        "second_up": jnp.clip(jnp.exp(math.log(9.99999993922529e-09) - 4.6051702 * jax.random.uniform(key_list[10], (D * FF,), jnp.float32) ** shard_levels(key_list[10], (D * FF,), ((0, 32),), -0.2, 0.2)), 1.000000013351432e-10, 9.99999993922529e-09),
        "second_down": jnp.clip(jnp.exp(math.log(9.99999993922529e-09) - 4.6051702 * jax.random.uniform(key_list[11], (FF * D,), jnp.float32) ** shard_levels(key_list[11], (FF * D,), ((0, 32),), -0.2, 0.2)), 1.000000013351432e-10, 9.99999993922529e-09),
        "second_out": jnp.clip(jnp.exp(math.log(9.99999993922529e-09) - 4.6051702 * jax.random.uniform(key_list[12], (D * VOCAB,), jnp.float32) ** shard_levels(key_list[12], (D * VOCAB,), ((0, 32),), -0.2, 0.2)), 1.000000013351432e-10, 9.99999993922529e-09),
    }


first_correction = 1.0 - (0.9 ** 10) ** 10
second_correction = 1.0 - (0.999 ** 10) ** 10

def ctc_losses(log_probs, labels, frame_lens, label_lens):
    batch, frames, vocab = log_probs.shape
    label_count = labels.shape[1]
    states = 2 * label_count + 1
    blanks = jnp.zeros_like(labels)
    extended = jnp.concatenate([jnp.stack([blanks, labels], axis=2).reshape(batch, 2 * label_count), blanks[:, :1]], axis=1)
    earlier = jnp.concatenate([jnp.full((batch, 2), -1, jnp.int32), extended[:, :-2]], axis=1)
    may_skip = (extended != 0) & (extended != earlier)
    onehot = (extended[:, :, None] == jnp.arange(vocab, dtype=jnp.int32)[None, None, :]).astype(log_probs.dtype)
    emitted = jnp.einsum('btv,bsv->tbs', log_probs, onehot, precision=lax.Precision.HIGHEST)
    state_ids = jnp.arange(states, dtype=jnp.int32)
    start = jnp.where(state_ids[None, :] < 2, emitted[0], -1e+30)
    frame_ids = jnp.arange(1, frames, dtype=jnp.int32)

    def advance(alpha, inputs):
        emit_row, frame_id = inputs
        lowest = jnp.full((batch, 1), -1e+30, alpha.dtype)
        from_one = jnp.concatenate([lowest, alpha[:, :-1]], axis=1)
        from_two = jnp.concatenate([lowest, lowest, alpha[:, :-2]], axis=1)
        from_two = jnp.where(may_skip, from_two, -1e+30)
        merged = jnp.logaddexp(jnp.logaddexp(alpha, from_one), from_two) + emit_row
        alive = frame_id < frame_lens[:, None]
        return (jnp.where(alive, merged, alpha), None)
    alpha, _ = lax.scan(advance, start, (emitted[1:], frame_ids))
    last_state = 2 * label_lens
    pick_end = lax.optimization_barrier(jnp.sum(jnp.where(state_ids[None, :] == last_state[:, None], alpha, 0.0), axis=1))
    pick_label = lax.optimization_barrier(jnp.sum(jnp.where(state_ids[None, :] == last_state[:, None] - 1, alpha, 0.0), axis=1))
    return -jnp.logaddexp(pick_end, pick_label)

def shard_gradients(features, frame_lens, labels, label_lens, up_mat, down_mat, out_mat, loss_scale):
    batch, frames, width = features.shape
    vocab = out_mat.shape[1]
    flat_in = features.reshape(batch * frames, width).astype(jnp.float32)
    centre = lax.optimization_barrier(jnp.mean(flat_in, axis=1, keepdims=True))
    spread = lax.optimization_barrier(jnp.mean((flat_in - centre) ** 2, axis=1, keepdims=True))
    normalized = ((flat_in - centre) * lax.rsqrt(spread + 1e-05)).astype(jnp.bfloat16)
    activation = jnp.dot(normalized, up_mat, preferred_element_type=jnp.float32)
    hidden = jax.nn.silu(activation).astype(jnp.bfloat16)
    block_out = (flat_in + 0.5 * jnp.dot(hidden, down_mat, preferred_element_type=jnp.float32)).astype(jnp.bfloat16)
    logits = jnp.dot(block_out, out_mat, preferred_element_type=jnp.float32)

    def loss_of(logit_rows):
        log_probs = jax.nn.log_softmax(logit_rows.reshape(batch, frames, vocab), axis=-1)
        return loss_scale * jnp.sum(ctc_losses(log_probs, labels, frame_lens, label_lens))
    loss_value, pullback = jax.vjp(loss_of, logits)
    logit_grad = pullback(jnp.ones((), loss_value.dtype))[0].astype(jnp.bfloat16)
    grad_out = jnp.dot(block_out.T, logit_grad, preferred_element_type=jnp.float32)
    ff_grad = (0.5 * jnp.dot(logit_grad, out_mat.T, preferred_element_type=jnp.float32)).astype(jnp.bfloat16)
    grad_down = jnp.dot(hidden.T, ff_grad, preferred_element_type=jnp.float32)
    sigmoid = jax.nn.sigmoid(activation)
    slope = sigmoid * (1.0 + activation * (1.0 - sigmoid))
    act_grad = (jnp.dot(ff_grad, down_mat.T, preferred_element_type=jnp.float32) * slope).astype(jnp.bfloat16)
    grad_up = jnp.dot(normalized.T, act_grad, preferred_element_type=jnp.float32)
    return (grad_up, grad_down, grad_out)

def adam_update(weight, first, second, grad, clip):
    scaled = clip * grad
    new_first = 0.9 * first + 0.1 * scaled
    new_second = 0.999 * second + 0.001 * scaled * scaled
    ratio = new_first / first_correction / (jnp.sqrt(new_second / second_correction) + 1e-08)
    return (weight - 0.001 * ratio, new_first, new_second)

def reference(features, frame_lens, labels, label_lens, w_up, w_down, w_out, first_up, first_down, first_out, second_up, second_down, second_out):
    up_mat = w_up.astype(jnp.bfloat16).reshape(D, FF)
    down_mat = w_down.astype(jnp.bfloat16).reshape(FF, D)
    out_mat = w_out.astype(jnp.bfloat16).reshape(D, VOCAB)
    loss_scale = 1.0 / (UTT * N_DP)
    shards = (features.reshape(N_DP, UTT, FRAMES, D), frame_lens.reshape(N_DP, UTT), labels.reshape(N_DP, UTT, LABELS), label_lens.reshape(N_DP, UTT))

    def accumulate(carry, item):
        terms = shard_gradients(item[0], item[1], item[2], item[3], up_mat, down_mat, out_mat, loss_scale)
        return ((carry[0] + terms[0], carry[1] + terms[1], carry[2] + terms[2]), None)
    start = (jnp.zeros((D, FF), jnp.float32), jnp.zeros((FF, D), jnp.float32), jnp.zeros((D, VOCAB), jnp.float32))
    sums, _ = lax.scan(accumulate, start, shards)
    grad_up = sums[0].reshape(-1)
    grad_down = sums[1].reshape(-1)
    grad_out = sums[2].reshape(-1)
    total = jnp.sum(grad_up * grad_up) + jnp.sum(grad_down * grad_down) + jnp.sum(grad_out * grad_out)
    clip = 1.0 / jnp.maximum(jnp.sqrt(total), 1.0)
    new_up, new_first_up, new_second_up = adam_update(w_up, first_up, second_up, grad_up, clip)
    new_down, new_first_down, new_second_down = adam_update(w_down, first_down, second_down, grad_down, clip)
    new_out, new_first_out, new_second_out = adam_update(w_out, first_out, second_out, grad_out, clip)
    return (new_up, new_down, new_out, new_first_up, new_first_down, new_first_out, new_second_up, new_second_down, new_second_out)
```

```python
import functools

import jax
import jax.numpy as jnp
from jax import lax
from jax.experimental import pallas as pl
from jax.experimental.pallas import tpu as pltpu
from jax.sharding import PartitionSpec as P

D = 256
FF = 1024
VOCAB = 256
LANES = 128
MESH = pl.DeviceIdType.MESH

first_correction = 1.0 - (0.9**10) ** 10
second_correction = 1.0 - (0.999**10) ** 10
negative = -1e30
VMEM = pl.BlockSpec(memory_space=pltpu.VMEM)
SMEM = pl.BlockSpec(memory_space=pltpu.SMEM)


def flip(me, bit):
    return me + bit - 2 * bit * ((me // bit) % 2)


def bit_orders(devices):
    bits = [1 << k for k in range(devices.bit_length() - 1)]
    core, rest = bits[:1], bits[1:]
    down = rest[::-1]
    swapped = down[:-2] + down[-2:][::-1]
    turned = down[-2:] + down[:-2]
    return (down + core, swapped + core, turned + core)


def subsets(bits):
    offsets = [0]
    for bit in bits:
        offsets = offsets + [offset + bit for offset in offsets]
    return offsets


def place_with(me, free, pattern):
    place = me
    for bit in free:
        if pattern & bit:
            place = flip(place, bit)
    return place


def gather_kernel(devices, w_up, w_down, w_out, full_up, full_down, full_out, send_sem, recv_sem):
    me = lax.axis_index("dp")
    orders = bit_orders(devices)
    barrier = pltpu.get_barrier_semaphore()
    for bit in orders[0]:
        pl.semaphore_signal(barrier, inc=1, device_id=(flip(me, bit),), device_id_type=MESH)
    fulls = (full_up, full_down, full_out)
    for shard, full in zip((w_up, w_down, w_out), fulls):
        rows, width = full.shape[1:]
        parts = width // LANES
        for part in range(parts):
            full[me, :, part * LANES : (part + 1) * LANES] = shard[
                pl.ds(part, rows, stride=parts), :
            ].astype(jnp.bfloat16)
    pl.semaphore_wait(barrier, len(orders[0]))

    copies = [{}, {}, {}]

    def send(which, pattern, stage):
        order, full = orders[which], fulls[which]
        owner = place_with(me, order[:stage], pattern)
        slot = pattern + order[stage]
        copy = pltpu.make_async_remote_copy(
            src_ref=full.at[owner],
            dst_ref=full.at[owner],
            send_sem=send_sem.at[which, slot],
            recv_sem=recv_sem.at[which, slot],
            device_id=(flip(me, order[stage]),),
            device_id_type=MESH,
        )
        copy.start()
        copies[which][slot] = copy

    steps = len(orders[0])
    for which in range(3):
        for stage in range(steps):
            send(which, 0, stage)
    for stage in range(steps):
        for pattern_at in range(1 << stage):
            for which in range(3):
                order = orders[which]
                pattern = subsets(order[:stage])[pattern_at] + order[stage]
                copies[which][pattern].wait_recv()
                for later in range(stage + 1, steps):
                    send(which, pattern, later)
    for which in range(3):
        for copy in copies[which].values():
            copy.wait_send()


def gather_weights(devices, w_up, w_down, w_out):
    shapes = []
    for shard, width in ((w_up, FF), (w_down, D), (w_out, VOCAB)):
        shapes.append(
            jax.ShapeDtypeStruct((devices, shard.size // width, width), jnp.bfloat16)
        )
    return pl.pallas_call(
        functools.partial(gather_kernel, devices),
        out_shape=shapes,
        in_specs=[VMEM] * 3,
        out_specs=[VMEM] * 3,
        scratch_shapes=[
            pltpu.SemaphoreType.DMA((3, devices)),
            pltpu.SemaphoreType.DMA((3, devices)),
        ],
        compiler_params=pltpu.CompilerParams(collective_id=0, has_side_effects=True),
        name="gather_weights",
    )(w_up, w_down, w_out)


def dot_rows(left, right):
    return jnp.dot(left, right, preferred_element_type=jnp.float32)


def dot_last(left, right, precision=None):
    return lax.dot_general(
        left, right, (((1,), (1,)), ((), ())), precision=precision,
        preferred_element_type=jnp.float32,
    )


def dot_first(left, right):
    return lax.dot_general(
        left, right, (((0,), (0,)), ((), ())), preferred_element_type=jnp.float32
    )


def step_kernel(
    loss_scale,
    frame_lens,
    label_lens,
    features,
    labels,
    up_mat,
    down_mat,
    out_mat,
    grad_up,
    grad_down,
    grad_out,
    normalized,
    activation,
    hidden,
    block_out,
    log_probs,
    emitted,
    alpha_rows,
    beta_rows,
    logit_grad,
    ff_grad,
    act_grad,
):
    utterances, label_count = labels.shape
    total = features.shape[0]
    frames = total // utterances
    states = 2 * label_count + 1
    block = min(128, total)

    @pl.loop(0, total // block)
    def _(step):
        rows = pl.ds(pl.multiple_of(step * block, block), block)
        flat_in = features[rows, :].astype(jnp.float32)
        centre = jnp.mean(flat_in, axis=1, keepdims=True)
        shifted = flat_in - centre
        spread = jnp.mean(shifted * shifted, axis=1, keepdims=True)
        norm = (shifted * lax.rsqrt(spread + 1e-05)).astype(jnp.bfloat16)
        normalized[rows, :] = norm
        act = dot_rows(norm, up_mat[...])
        activation[rows, :] = act
        hid = (act * (1.0 / (1.0 + jnp.exp(-act)))).astype(jnp.bfloat16)
        hidden[rows, :] = hid
        out_rows = (flat_in + 0.5 * dot_rows(hid, down_mat[...])).astype(jnp.bfloat16)
        block_out[rows, :] = out_rows
        logits = dot_rows(out_rows, out_mat[...])
        top = jnp.max(logits, axis=1, keepdims=True)
        low = logits - top
        log_probs[rows, :] = low - jnp.log(jnp.sum(jnp.exp(low), axis=1, keepdims=True))

    label_ids = lax.broadcasted_iota(jnp.int32, (label_count, LANES), 0)
    state_at = lax.broadcasted_iota(jnp.int32, (label_count, LANES), 1)
    spread_now = (state_at == 2 * label_ids + 1).astype(jnp.bfloat16)
    spread_back = (state_at == 2 * label_ids + 3).astype(jnp.bfloat16)
    spread_ahead = (state_at == 2 * label_ids - 1).astype(jnp.bfloat16)
    label_rows = jnp.concatenate(
        [
            labels[...].astype(jnp.float32),
            jnp.zeros((8 - utterances, label_count), jnp.float32),
        ],
        axis=0,
    ).astype(jnp.bfloat16)
    extended = dot_rows(label_rows, spread_now)
    earlier = dot_rows(label_rows, spread_back)
    later = dot_rows(label_rows, spread_ahead)
    row_ids = lax.broadcasted_iota(jnp.int32, (8, LANES), 0)
    lane_ids = lax.broadcasted_iota(jnp.int32, (8, LANES), 1)
    may_skip = (extended > 0.5) & (extended != earlier)
    skip_later = (later > 0.5) & (later != extended)
    skip_add = jnp.where(may_skip, 0.0, negative)
    later_add = jnp.where(skip_later, 0.0, negative)
    start = jnp.where(lane_ids < 2, 0.0, negative)
    ends = jnp.full((8, LANES), -9, jnp.int32)
    first_frame = jnp.full((8, LANES), -9, jnp.int32)
    for utterance in range(utterances):
        ends = jnp.where(row_ids == utterance, 2 * label_lens[utterance], ends)
        first_frame = jnp.where(row_ids == utterance, frame_lens[utterance] - 1, first_frame)
    finish = jnp.where((lane_ids == ends) | (lane_ids == ends - 1), 0.0, negative)

    emitted[...] = jnp.full(emitted.shape, negative, jnp.float32)
    vocab_ids = lax.broadcasted_iota(jnp.int32, (VOCAB, LANES), 0).astype(jnp.float32)
    lanes_wide = lax.broadcasted_iota(jnp.int32, (VOCAB, LANES), 1)
    frame_lanes = lax.broadcasted_iota(jnp.int32, (frames, LANES), 1)
    onehots = []
    for utterance in range(utterances):
        onehot = jnp.where(
            (vocab_ids == extended[utterance : utterance + 1, :]) & (lanes_wide < states), 1.0, 0.0
        )
        onehots.append(onehot)
        picked = jnp.dot(
            log_probs[utterance * frames : (utterance + 1) * frames, :],
            onehot,
            precision=lax.Precision.HIGHEST,
            preferred_element_type=jnp.float32,
        )
        emitted[:, utterance, :] = jnp.where(frame_lanes < states, picked, negative)

    def log_three(one, two, three):
        top = jnp.maximum(jnp.maximum(one, two), three)
        return top + jnp.log(jnp.exp(one - top) + jnp.exp(two - top) + jnp.exp(three - top))

    def advance(frame, carry):
        alpha, weighted = carry
        back = frames - 1 - frame
        base = log_three(
            alpha, pltpu.roll(alpha, 1, 1), pltpu.roll(alpha, 2, 1) + skip_add
        )
        base = jnp.where(jnp.full((8, LANES), frame, jnp.int32) == 0, start, base)
        other = log_three(
            weighted,
            pltpu.roll(weighted, LANES - 1, 1),
            pltpu.roll(weighted, LANES - 2, 1) + later_add,
        )
        other = jnp.where(first_frame == back, finish, other)
        alpha_rows[frame] = base
        beta_rows[back] = other
        return (base + emitted[frame], other + emitted[back])

    nothing = jnp.full((8, LANES), negative, jnp.float32)
    lax.fori_loop(0, frames, advance, (nothing, nothing), unroll=8)

    frame_ids = lax.broadcasted_iota(jnp.int32, (frames, LANES), 0)
    for utterance in range(utterances):
        joint = (
            alpha_rows[:, utterance, :] + emitted[:, utterance, :] + beta_rows[:, utterance, :]
        )
        top = jnp.max(joint, axis=1, keepdims=True)
        mass = jnp.exp(joint - top)
        share = mass / jnp.sum(mass, axis=1, keepdims=True)
        occupancy = jnp.where(frame_ids < frame_lens[utterance], share, 0.0)
        gamma = dot_last(occupancy, onehots[utterance], lax.Precision.HIGHEST)
        rows = slice(utterance * frames, (utterance + 1) * frames)
        probs = jnp.exp(log_probs[rows, :])
        held = jnp.sum(occupancy, axis=1, keepdims=True)
        logit_grad[rows, :] = (loss_scale * (probs * held - gamma)).astype(jnp.bfloat16)

    @pl.loop(0, total // block)
    def _(step):
        rows = pl.ds(pl.multiple_of(step * block, block), block)
        grad_rows = (0.5 * dot_last(logit_grad[rows, :], out_mat[...])).astype(jnp.bfloat16)
        ff_grad[rows, :] = grad_rows
        act = activation[rows, :]
        sigmoid = 1.0 / (1.0 + jnp.exp(-act))
        slope = sigmoid * (1.0 + act * (1.0 - sigmoid))
        act_grad[rows, :] = (dot_last(grad_rows, down_mat[...]) * slope).astype(jnp.bfloat16)

    grad_up[...] = dot_first(normalized[...], act_grad[...])
    grad_down[...] = dot_first(hidden[...], ff_grad[...])
    grad_out[...] = dot_first(block_out[...], logit_grad[...])


def local_step(loss_scale, frame_lens, label_lens, features, labels, up_mat, down_mat, out_mat):
    total = features.shape[0]
    frames = total // labels.shape[0]
    return pl.pallas_call(
        functools.partial(step_kernel, loss_scale),
        out_shape=[
            jax.ShapeDtypeStruct((D, FF), jnp.float32),
            jax.ShapeDtypeStruct((FF, D), jnp.float32),
            jax.ShapeDtypeStruct((D, VOCAB), jnp.float32),
        ],
        in_specs=[SMEM, SMEM] + [VMEM] * 5,
        out_specs=[VMEM] * 3,
        scratch_shapes=[
            pltpu.VMEM((total, D), jnp.bfloat16),
            pltpu.VMEM((total, FF), jnp.float32),
            pltpu.VMEM((total, FF), jnp.bfloat16),
            pltpu.VMEM((total, D), jnp.bfloat16),
            pltpu.VMEM((total, VOCAB), jnp.float32),
            pltpu.VMEM((frames, 8, LANES), jnp.float32),
            pltpu.VMEM((frames, 8, LANES), jnp.float32),
            pltpu.VMEM((frames, 8, LANES), jnp.float32),
            pltpu.VMEM((total, VOCAB), jnp.bfloat16),
            pltpu.VMEM((total, D), jnp.bfloat16),
            pltpu.VMEM((total, FF), jnp.bfloat16),
        ],
        compiler_params=pltpu.CompilerParams(vmem_limit_bytes=40 << 20),
        name="local_step",
    )(frame_lens, label_lens, features, labels, up_mat, down_mat, out_mat)


def sum_kernel(devices, *refs):
    grads, reduced, squares = refs[:3], refs[3:6], refs[6]
    received, staged = refs[7:10], refs[10:13]
    own_squares, send_sem, recv_sem, small_send, small_recv = refs[13:]
    me = lax.axis_index("dp")
    orders = [order[::-1] for order in bit_orders(devices)]
    steps = len(orders[0])
    barrier = pltpu.get_barrier_semaphore()

    @pl.loop(1, devices)
    def _(shift):
        pl.semaphore_signal(
            barrier, inc=1, device_id=((me + shift) % devices,), device_id_type=MESH
        )

    pl.semaphore_wait(barrier, devices - 1)

    copies = [{}, {}, {}]

    def sum_of(which, place, pattern, stage):
        value = grads[which][place]
        order = orders[which]
        for past in range(stage):
            slot = pattern + order[past]
            copies[which][slot].wait_recv()
            value = value + received[which][slot]
        return value

    for stage in range(steps):
        for at in range(1 << (steps - 1 - stage)):
            for which in range(3):
                order = orders[which]
                rest = order[stage + 1 :]
                pattern = subsets(rest[::-1])[::-1][at] + order[stage]
                place = place_with(me, order, pattern)
                landing = pattern - order[stage]
                if stage == 0:
                    source = grads[which].at[place]
                else:
                    staged[which][pattern] = sum_of(which, place, pattern, stage)
                    source = staged[which].at[pattern]
                slot = landing + order[stage]
                copy = pltpu.make_async_remote_copy(
                    src_ref=source,
                    dst_ref=received[which].at[slot],
                    send_sem=send_sem.at[which, slot],
                    recv_sem=recv_sem.at[which, slot],
                    device_id=(flip(me, order[stage]),),
                    device_id_type=MESH,
                )
                copy.start()
                copies[which][slot] = copy

    own = jnp.zeros((1, LANES), jnp.float32)
    for which in range(3):
        value = sum_of(which, me, 0, steps)
        rows, width = value.shape
        parts = width // LANES
        for part in range(parts):
            piece = value[:, part * LANES : (part + 1) * LANES]
            reduced[which][pl.ds(part, rows, stride=parts), :] = piece
            own = own + jnp.sum(piece * piece, axis=0, keepdims=True)
    own_squares[...] = own
    squares[0] = own

    def small_copy(shift):
        return pltpu.make_async_remote_copy(
            src_ref=own_squares,
            dst_ref=squares.at[shift],
            send_sem=small_send.at[shift],
            recv_sem=small_recv.at[shift],
            device_id=((me + shift) % devices,),
            device_id_type=MESH,
        )

    @pl.loop(1, devices)
    def _(shift):
        small_copy(shift).start()

    for which in range(3):
        for copy in copies[which].values():
            copy.wait_send()

    @pl.loop(1, devices)
    def _(shift):
        small_copy(shift).wait()


def sum_gradients(devices, grads):
    blocks = [grad.reshape(devices, grad.shape[0] // devices, grad.shape[1]) for grad in grads]
    shapes = [
        jax.ShapeDtypeStruct((block[0].size // LANES, LANES), jnp.float32) for block in blocks
    ]
    buffers = [pltpu.VMEM(block.shape, jnp.float32) for block in blocks]
    return pl.pallas_call(
        functools.partial(sum_kernel, devices),
        out_shape=shapes + [jax.ShapeDtypeStruct((devices, 1, LANES), jnp.float32)],
        in_specs=[VMEM] * 3,
        out_specs=[VMEM] * 4,
        scratch_shapes=buffers
        + buffers
        + [
            pltpu.VMEM((1, LANES), jnp.float32),
            pltpu.SemaphoreType.DMA((3, devices)),
            pltpu.SemaphoreType.DMA((3, devices)),
            pltpu.SemaphoreType.DMA((devices,)),
            pltpu.SemaphoreType.DMA((devices,)),
        ],
        compiler_params=pltpu.CompilerParams(
            collective_id=1, has_side_effects=True, vmem_limit_bytes=50 << 20
        ),
        name="sum_gradients",
    )(*blocks)


def adam_kernel(squares, *refs):
    weights, firsts, seconds, grads, outs = (refs[at : at + 3] for at in (0, 3, 6, 9, 12))
    new_firsts, new_seconds = refs[15:18], refs[18:21]
    total = jnp.sum(squares[...])
    clip = 1.0 / jnp.maximum(jnp.sqrt(jnp.full((1, LANES), total)), 1.0)
    for which in range(3):
        scaled = clip * grads[which][...]
        first = 0.9 * firsts[which][...] + 0.1 * scaled
        second = 0.999 * seconds[which][...] + 0.001 * scaled * scaled
        ratio = first / first_correction / (jnp.sqrt(second / second_correction) + 1e-08)
        outs[which][...] = weights[which][...] - 0.001 * ratio
        new_firsts[which][...] = first
        new_seconds[which][...] = second


def adam(squares, weights, firsts, seconds, grads):
    shapes = [jax.ShapeDtypeStruct(weight.shape, jnp.float32) for weight in weights]
    return pl.pallas_call(
        adam_kernel,
        out_shape=shapes * 3,
        in_specs=[VMEM] * 13,
        out_specs=[VMEM] * 9,
        name="adam",
    )(squares, *weights, *firsts, *seconds, *grads)


def per_device(
    features,
    frame_lens,
    labels,
    label_lens,
    w_up,
    w_down,
    w_out,
    first_up,
    first_down,
    first_out,
    second_up,
    second_down,
    second_out,
):
    devices = lax.axis_size("dp")
    batch, frames, width = features.shape

    def lined(*arrays):
        return [array.reshape(array.shape[0] // LANES, LANES) for array in arrays]

    weights = lined(w_up, w_down, w_out)
    full_up, full_down, full_out = gather_weights(devices, *weights)
    grads = local_step(
        1.0 / (batch * devices),
        frame_lens,
        label_lens,
        features.reshape(batch * frames, width),
        labels,
        full_up.reshape(D, FF),
        full_down.reshape(FF, D),
        full_out.reshape(D, VOCAB),
    )
    *shares, squares = sum_gradients(devices, grads)
    results = adam(
        squares,
        weights,
        lined(first_up, first_down, first_out),
        lined(second_up, second_down, second_out),
        shares,
    )
    return tuple(result.reshape(-1) for result in results)


def solution(mesh):
    flat = P("dp")
    return jax.shard_map(
        per_device,
        mesh=mesh,
        in_specs=(P("dp", None, None), flat, P("dp", None), flat) + (flat,) * 9,
        out_specs=(flat,) * 9,
        check_vma=False,
    )
```

```python
import functools

import jax
import jax.numpy as jnp
from jax import lax
from jax.experimental import pallas as pl
from jax.experimental.pallas import tpu as pltpu
from jax.sharding import PartitionSpec as P

D = 256
FF = 1024
VOCAB = 256
LANES = 128
MESH = pl.DeviceIdType.MESH

first_correction = 1.0 - (0.9**10) ** 10
second_correction = 1.0 - (0.999**10) ** 10
negative = -1e30
VMEM = pl.BlockSpec(memory_space=pltpu.VMEM)
SMEM = pl.BlockSpec(memory_space=pltpu.SMEM)


def flip(me, bit):
    return me + bit - 2 * bit * ((me // bit) % 2)


def bit_orders(devices):
    bits = [1 << k for k in range(devices.bit_length() - 1)]
    core, rest = bits[:1], bits[1:]
    down = rest[::-1]
    swapped = down[:-2] + down[-2:][::-1]
    turned = down[-2:] + down[:-2]
    return (down + core, swapped + core, turned + core)


def subsets(bits):
    offsets = [0]
    for bit in bits:
        offsets = offsets + [offset + bit for offset in offsets]
    return offsets


def place_with(me, free, pattern):
    place = me
    for bit in free:
        if pattern & bit:
            place = flip(place, bit)
    return place


class Gather:
    def __init__(self, me, devices, fulls, send_sem, recv_sem):
        self.me, self.fulls = me, fulls
        self.send_sem, self.recv_sem = send_sem, recv_sem
        self.orders = bit_orders(devices)
        self.steps = len(self.orders[0])
        self.copies = [{}, {}, {}]

    def fill(self, shards):
        for shard, full in zip(shards, self.fulls):
            rows, width = full.shape[1:]
            parts = width // LANES
            for part in range(parts):
                full[self.me, :, part * LANES : (part + 1) * LANES] = shard[
                    pl.ds(part, rows, stride=parts), :
                ].astype(jnp.bfloat16)

    def send(self, which, pattern, stage):
        order, full = self.orders[which], self.fulls[which]
        owner = place_with(self.me, order[:stage], pattern)
        slot = pattern + order[stage]
        copy = pltpu.make_async_remote_copy(
            src_ref=full.at[owner],
            dst_ref=full.at[owner],
            send_sem=self.send_sem.at[which, slot],
            recv_sem=self.recv_sem.at[which, slot],
            device_id=(flip(self.me, order[stage]),),
            device_id_type=MESH,
        )
        copy.start()
        self.copies[which][slot] = copy

    def pass_on(self):
        for which in range(3):
            for stage in range(self.steps):
                self.send(which, 0, stage)
        for stage in range(self.steps - 1):
            for at in range(1 << stage):
                for which in range(3):
                    order = self.orders[which]
                    pattern = subsets(order[:stage])[at] + order[stage]
                    self.copies[which][pattern].wait_recv()
                    for later in range(stage + 1, self.steps):
                        self.send(which, pattern, later)

    def arrive(self, which):
        order = self.orders[which]
        for pattern in subsets(order[:-1]):
            self.copies[which][pattern + order[-1]].wait_recv()

    def close(self):
        for copies in self.copies:
            for copy in copies.values():
                copy.wait_send()


def greet(me, devices, barrier):
    @pl.loop(1, devices)
    def _(shift):
        pl.semaphore_signal(
            barrier, inc=1, device_id=((me + shift) % devices,), device_id_type=MESH
        )


def gather_kernel(devices, w_up, w_down, w_out, full_up, full_down, full_out, send_sem, recv_sem):
    me = lax.axis_index("dp")
    barrier = pltpu.get_barrier_semaphore()
    greet(me, devices, barrier)
    gather = Gather(me, devices, (full_up, full_down, full_out), send_sem, recv_sem)
    gather.fill((w_up, w_down, w_out))
    pl.semaphore_wait(barrier, devices - 1)
    gather.pass_on()
    for which in range(3):
        gather.arrive(which)
    gather.close()


def gather_weights(devices, w_up, w_down, w_out):
    shapes = []
    for shard, width in ((w_up, FF), (w_down, D), (w_out, VOCAB)):
        shapes.append(
            jax.ShapeDtypeStruct((devices, shard.size // width, width), jnp.bfloat16)
        )
    return pl.pallas_call(
        functools.partial(gather_kernel, devices),
        out_shape=shapes,
        in_specs=[VMEM] * 3,
        out_specs=[VMEM] * 3,
        scratch_shapes=[
            pltpu.SemaphoreType.DMA((3, devices)),
            pltpu.SemaphoreType.DMA((3, devices)),
        ],
        compiler_params=pltpu.CompilerParams(collective_id=0, has_side_effects=True),
        name="gather_weights",
    )(w_up, w_down, w_out)


def dot_rows(left, right):
    return jnp.dot(left, right, preferred_element_type=jnp.float32)


def dot_last(left, right, precision=None):
    return lax.dot_general(
        left, right, (((1,), (1,)), ((), ())), precision=precision,
        preferred_element_type=jnp.float32,
    )


def dot_first(left, right):
    return lax.dot_general(
        left, right, (((0,), (0,)), ((), ())), preferred_element_type=jnp.float32
    )


def row_blocks(total, body):
    block = min(128, total)

    @pl.loop(0, total // block)
    def _(step):
        body(pl.ds(pl.multiple_of(step * block, block), block))


def normalize(features, normalized):
    def body(rows):
        flat_in = features[rows, :].astype(jnp.float32)
        centre = jnp.mean(flat_in, axis=1, keepdims=True)
        shifted = flat_in - centre
        spread = jnp.mean(shifted * shifted, axis=1, keepdims=True)
        normalized[rows, :] = (shifted * lax.rsqrt(spread + 1e-05)).astype(jnp.bfloat16)

    row_blocks(features.shape[0], body)


def project_up(normalized, up_mat, activation, hidden):
    def body(rows):
        act = dot_rows(normalized[rows, :], up_mat[...].reshape(D, FF))
        activation[rows, :] = act
        hidden[rows, :] = (act * (1.0 / (1.0 + jnp.exp(-act)))).astype(jnp.bfloat16)

    row_blocks(normalized.shape[0], body)


def project_down(features, hidden, down_mat, out_mat, block_out, log_probs):
    def body(rows):
        flat_in = features[rows, :].astype(jnp.float32)
        out_rows = (flat_in + 0.5 * dot_rows(hidden[rows, :], down_mat[...].reshape(FF, D))).astype(
            jnp.bfloat16
        )
        block_out[rows, :] = out_rows
        logits = dot_rows(out_rows, out_mat[...].reshape(D, VOCAB))
        top = jnp.max(logits, axis=1, keepdims=True)
        low = logits - top
        log_probs[rows, :] = low - jnp.log(jnp.sum(jnp.exp(low), axis=1, keepdims=True))

    row_blocks(features.shape[0], body)


def ctc_grad(
    loss_scale,
    frame_lens,
    label_lens,
    labels,
    log_probs,
    emitted,
    alpha_rows,
    beta_rows,
    logit_grad,
):
    utterances, label_count = labels.shape
    frames = log_probs.shape[0] // utterances
    states = 2 * label_count + 1

    label_ids = lax.broadcasted_iota(jnp.int32, (label_count, LANES), 0)
    state_at = lax.broadcasted_iota(jnp.int32, (label_count, LANES), 1)
    spread_now = (state_at == 2 * label_ids + 1).astype(jnp.bfloat16)
    spread_back = (state_at == 2 * label_ids + 3).astype(jnp.bfloat16)
    spread_ahead = (state_at == 2 * label_ids - 1).astype(jnp.bfloat16)
    label_rows = jnp.concatenate(
        [
            labels[...].astype(jnp.float32),
            jnp.zeros((8 - utterances, label_count), jnp.float32),
        ],
        axis=0,
    ).astype(jnp.bfloat16)
    extended = dot_rows(label_rows, spread_now)
    earlier = dot_rows(label_rows, spread_back)
    later = dot_rows(label_rows, spread_ahead)
    row_ids = lax.broadcasted_iota(jnp.int32, (8, LANES), 0)
    lane_ids = lax.broadcasted_iota(jnp.int32, (8, LANES), 1)
    may_skip = (extended > 0.5) & (extended != earlier)
    skip_later = (later > 0.5) & (later != extended)
    skip_add = jnp.where(may_skip, 0.0, negative)
    later_add = jnp.where(skip_later, 0.0, negative)
    ends = jnp.full((8, LANES), -9, jnp.int32)
    first_frame = jnp.full((8, LANES), -9, jnp.int32)
    for utterance in range(utterances):
        ends = jnp.where(row_ids == utterance, 2 * label_lens[utterance], ends)
        first_frame = jnp.where(row_ids == utterance, frame_lens[utterance] - 1, first_frame)
    finish = jnp.where((lane_ids == ends) | (lane_ids == ends - 1), 0.0, negative)

    emitted[...] = jnp.full(emitted.shape, negative, jnp.float32)
    vocab_ids = lax.broadcasted_iota(jnp.int32, (VOCAB, LANES), 0).astype(jnp.float32)
    lanes_wide = lax.broadcasted_iota(jnp.int32, (VOCAB, LANES), 1)
    frame_lanes = lax.broadcasted_iota(jnp.int32, (frames, LANES), 1)
    onehots = []
    for utterance in range(utterances):
        onehot = jnp.where(
            (vocab_ids == extended[utterance : utterance + 1, :]) & (lanes_wide < states), 1.0, 0.0
        )
        onehots.append(onehot)
        picked = jnp.dot(
            log_probs[utterance * frames : (utterance + 1) * frames, :],
            onehot,
            precision=lax.Precision.HIGHEST,
            preferred_element_type=jnp.float32,
        )
        emitted[:, utterance, :] = jnp.where(frame_lanes < states, picked, negative)

    def log_three(one, two, three):
        top = jnp.maximum(jnp.maximum(one, two), three)
        return top + jnp.log(jnp.exp(one - top) + jnp.exp(two - top) + jnp.exp(three - top))

    def ahead(values, count):
        return pltpu.roll(values, count, 1) if count else values

    def behind(values, count):
        return pltpu.roll(values, LANES - count, 1) if count else values

    skips = [ahead(skip_add, count) for count in range(3)]
    later_skips = [behind(later_add, count) for count in range(3)]
    finishes = [behind(finish, count) for count in range(3)]

    def advance(pair, carry):
        alpha, weighted = carry
        frame = 2 * pair
        back = frames - 1 - frame
        moved = [ahead(alpha, count) for count in range(5)]
        other = [behind(weighted, count) for count in range(5)]
        emit, emit_back = emitted[frame], emitted[back]
        ends_here = first_frame == back
        firsts, lasts = [], []
        for count in range(3):
            base = log_three(moved[count], moved[count + 1], moved[count + 2] + skips[count])
            rest = log_three(other[count], other[count + 1], other[count + 2] + later_skips[count])
            rest = jnp.where(ends_here, finishes[count], rest)
            if count == 0:
                alpha_rows[frame] = base
                beta_rows[back] = rest
            firsts.append(base + ahead(emit, count))
            lasts.append(rest + behind(emit_back, count))
        base = log_three(firsts[0], firsts[1], firsts[2] + skips[0])
        rest = log_three(lasts[0], lasts[1], lasts[2] + later_skips[0])
        rest = jnp.where(first_frame == back - 1, finish, rest)
        alpha_rows[frame + 1] = base
        beta_rows[back - 1] = rest
        return (base + emitted[frame + 1], rest + emitted[back - 1])

    nothing = jnp.full((8, LANES), negative, jnp.float32)
    start = jnp.where(lane_ids == 0, 0.0, negative)
    lax.fori_loop(0, frames // 2, advance, (start, nothing), unroll=4)

    frame_ids = lax.broadcasted_iota(jnp.int32, (frames, LANES), 0)
    for utterance in range(utterances):
        joint = (
            alpha_rows[:, utterance, :] + emitted[:, utterance, :] + beta_rows[:, utterance, :]
        )
        top = jnp.max(joint, axis=1, keepdims=True)
        mass = jnp.exp(joint - top)
        share = mass / jnp.sum(mass, axis=1, keepdims=True)
        occupancy = jnp.where(frame_ids < frame_lens[utterance], share, 0.0)
        gamma = dot_last(occupancy, onehots[utterance], lax.Precision.HIGHEST)
        rows = slice(utterance * frames, (utterance + 1) * frames)
        probs = jnp.exp(log_probs[rows, :])
        held = jnp.sum(occupancy, axis=1, keepdims=True)
        logit_grad[rows, :] = (loss_scale * (probs * held - gamma)).astype(jnp.bfloat16)


def grad_ff(logit_grad, out_mat, ff_grad):
    def body(rows):
        ff_grad[rows, :] = (
            0.5 * dot_last(logit_grad[rows, :], out_mat[...].reshape(D, VOCAB))
        ).astype(jnp.bfloat16)

    row_blocks(logit_grad.shape[0], body)


def grad_act(ff_grad, down_mat, activation, act_grad):
    def body(rows):
        act = activation[rows, :]
        sigmoid = 1.0 / (1.0 + jnp.exp(-act))
        slope = sigmoid * (1.0 + act * (1.0 - sigmoid))
        act_grad[rows, :] = (
            dot_last(ff_grad[rows, :], down_mat[...].reshape(FF, D)) * slope
        ).astype(jnp.bfloat16)

    row_blocks(ff_grad.shape[0], body)


def step_kernel(
    loss_scale,
    frame_lens,
    label_lens,
    features,
    labels,
    up_mat,
    down_mat,
    out_mat,
    grad_up,
    grad_down,
    grad_out,
    normalized,
    activation,
    hidden,
    block_out,
    log_probs,
    emitted,
    alpha_rows,
    beta_rows,
    logit_grad,
    ff_grad,
    act_grad,
):
    normalize(features, normalized)
    project_up(normalized, up_mat, activation, hidden)
    project_down(features, hidden, down_mat, out_mat, block_out, log_probs)
    ctc_grad(
        loss_scale, frame_lens, label_lens, labels, log_probs, emitted, alpha_rows, beta_rows,
        logit_grad,
    )
    grad_ff(logit_grad, out_mat, ff_grad)
    grad_act(ff_grad, down_mat, activation, act_grad)
    grad_up[...] = dot_first(normalized[...], act_grad[...])
    grad_down[...] = dot_first(hidden[...], ff_grad[...])
    grad_out[...] = dot_first(block_out[...], logit_grad[...])


def step_scratch(total, frames):
    return [
        pltpu.VMEM((total, D), jnp.bfloat16),
        pltpu.VMEM((total, FF), jnp.float32),
        pltpu.VMEM((total, FF), jnp.bfloat16),
        pltpu.VMEM((total, D), jnp.bfloat16),
        pltpu.VMEM((total, VOCAB), jnp.float32),
        pltpu.VMEM((frames, 8, LANES), jnp.float32),
        pltpu.VMEM((frames, 8, LANES), jnp.float32),
        pltpu.VMEM((frames, 8, LANES), jnp.float32),
        pltpu.VMEM((total, VOCAB), jnp.bfloat16),
        pltpu.VMEM((total, D), jnp.bfloat16),
        pltpu.VMEM((total, FF), jnp.bfloat16),
    ]


def local_step(loss_scale, frame_lens, label_lens, features, labels, up_mat, down_mat, out_mat):
    total = features.shape[0]
    frames = total // labels.shape[0]
    return pl.pallas_call(
        functools.partial(step_kernel, loss_scale),
        out_shape=[
            jax.ShapeDtypeStruct((D, FF), jnp.float32),
            jax.ShapeDtypeStruct((FF, D), jnp.float32),
            jax.ShapeDtypeStruct((D, VOCAB), jnp.float32),
        ],
        in_specs=[SMEM, SMEM] + [VMEM] * 5,
        out_specs=[VMEM] * 3,
        scratch_shapes=step_scratch(total, frames),
        compiler_params=pltpu.CompilerParams(vmem_limit_bytes=40 << 20),
        name="local_step",
    )(frame_lens, label_lens, features, labels, up_mat, down_mat, out_mat)


class Sum:
    def __init__(self, me, devices, grads, received, staged, send_sem, recv_sem):
        self.me, self.grads, self.received, self.staged = me, grads, received, staged
        self.send_sem, self.recv_sem = send_sem, recv_sem
        self.orders = [order[::-1] for order in bit_orders(devices)]
        self.steps = len(self.orders[0])
        self.copies = [{}, {}, {}]

    def sum_of(self, which, place, pattern, stage):
        value = self.grads[which][place]
        for bit in self.orders[which][:stage]:
            self.copies[which][pattern + bit].wait_recv()
            value = value + self.received[which][pattern + bit]
        return value

    def send(self, which, stage):
        order = self.orders[which]
        for offset in subsets(order[stage + 1 :][::-1])[::-1]:
            slot = offset + order[stage]
            place = place_with(self.me, order, slot)
            if stage == 0:
                source = self.grads[which].at[place]
            else:
                self.staged[which][slot] = self.sum_of(which, place, slot, stage)
                source = self.staged[which].at[slot]
            copy = pltpu.make_async_remote_copy(
                src_ref=source,
                dst_ref=self.received[which].at[slot],
                send_sem=self.send_sem.at[which, slot],
                recv_sem=self.recv_sem.at[which, slot],
                device_id=(flip(self.me, order[stage]),),
                device_id_type=MESH,
            )
            copy.start()
            self.copies[which][slot] = copy

    def finish(self, devices, reduced, squares, own_squares, small_send, small_recv):
        me = self.me
        own = jnp.zeros((1, LANES), jnp.float32)
        for which in (2, 1, 0):
            value = self.sum_of(which, me, 0, self.steps)
            rows, width = value.shape
            parts = width // LANES
            for part in range(parts):
                piece = value[:, part * LANES : (part + 1) * LANES]
                reduced[which][pl.ds(part, rows, stride=parts), :] = piece
                own = own + jnp.sum(piece * piece, axis=0, keepdims=True)
        own_squares[...] = own
        squares[0] = own

        def small_copy(shift):
            return pltpu.make_async_remote_copy(
                src_ref=own_squares,
                dst_ref=squares.at[shift],
                send_sem=small_send.at[shift],
                recv_sem=small_recv.at[shift],
                device_id=((me + shift) % devices,),
                device_id_type=MESH,
            )

        @pl.loop(1, devices)
        def _(shift):
            small_copy(shift).start()

        for copies in self.copies:
            for copy in copies.values():
                copy.wait_send()

        @pl.loop(1, devices)
        def _(shift):
            small_copy(shift).wait()


def sum_kernel(devices, *refs):
    grads, reduced, squares = refs[:3], refs[3:6], refs[6]
    received, staged = refs[7:10], refs[10:13]
    own_squares, send_sem, recv_sem, small_send, small_recv = refs[13:]
    me = lax.axis_index("dp")
    barrier = pltpu.get_barrier_semaphore()
    greet(me, devices, barrier)
    pl.semaphore_wait(barrier, devices - 1)
    total = Sum(me, devices, grads, received, staged, send_sem, recv_sem)
    for stage in range(total.steps):
        for which in range(3):
            total.send(which, stage)
    total.finish(devices, reduced, squares, own_squares, small_send, small_recv)


def fused_kernel(devices, loss_scale, *refs):
    frame_lens, label_lens, features, labels = refs[:4]
    shards, reduced, squares = refs[4:7], refs[7:10], refs[10]
    fulls, grads, received, staged = refs[11:14], refs[14:17], refs[17:20], refs[20:23]
    gather_send, gather_recv, own_squares, send_sem, recv_sem, small_send, small_recv = refs[23:30]
    normalized, activation, hidden, block_out, log_probs = refs[30:35]
    emitted, alpha_rows, beta_rows, logit_grad, ff_grad, act_grad = refs[35:]
    up_mat, down_mat, out_mat = fulls
    me = lax.axis_index("dp")
    barrier = pltpu.get_barrier_semaphore()
    greet(me, devices, barrier)
    gather = Gather(me, devices, fulls, gather_send, gather_recv)
    gather.fill(shards)
    normalize(features, normalized)
    pl.semaphore_wait(barrier, devices - 1)
    gather.pass_on()
    gather.arrive(0)
    project_up(normalized, up_mat, activation, hidden)
    gather.arrive(1)
    gather.arrive(2)
    project_down(features, hidden, down_mat, out_mat, block_out, log_probs)
    ctc_grad(
        loss_scale, frame_lens, label_lens, labels, log_probs, emitted, alpha_rows, beta_rows,
        logit_grad,
    )
    total = Sum(me, devices, grads, received, staged, send_sem, recv_sem)
    pending = [list(range(total.steps)) for _ in range(3)]

    def advance(*whiches):
        for which in whiches:
            if pending[which]:
                total.send(which, pending[which].pop(0))

    def put(which, value):
        grads[which][...] = value.reshape(grads[which].shape)

    grad_ff(logit_grad, out_mat, ff_grad)
    put(1, dot_first(hidden[...], ff_grad[...]))
    advance(1)
    grad_act(ff_grad, down_mat, activation, act_grad)
    advance(1)
    put(0, dot_first(normalized[...], act_grad[...]))
    advance(0)
    put(2, dot_first(block_out[...], logit_grad[...]))
    advance(2)
    while any(pending):
        advance(1, 0, 2)
    total.finish(devices, reduced, squares, own_squares, small_send, small_recv)
    gather.close()


def fused_step(loss_scale, devices, frame_lens, label_lens, features, labels, weights):
    total = features.shape[0]
    frames = total // labels.shape[0]
    blocks = [
        (devices, weight.size // width, width)
        for weight, width in zip(weights, (FF, D, VOCAB))
    ]
    wide = [pltpu.VMEM(block, jnp.float32) for block in blocks]
    return pl.pallas_call(
        functools.partial(fused_kernel, devices, loss_scale),
        out_shape=[jax.ShapeDtypeStruct(weight.shape, jnp.float32) for weight in weights]
        + [jax.ShapeDtypeStruct((devices, 1, LANES), jnp.float32)],
        in_specs=[SMEM, SMEM] + [VMEM] * 5,
        out_specs=[VMEM] * 4,
        scratch_shapes=[pltpu.VMEM(block, jnp.bfloat16) for block in blocks]
        + wide * 3
        + [
            pltpu.SemaphoreType.DMA((3, devices)),
            pltpu.SemaphoreType.DMA((3, devices)),
            pltpu.VMEM((1, LANES), jnp.float32),
            pltpu.SemaphoreType.DMA((3, devices)),
            pltpu.SemaphoreType.DMA((3, devices)),
            pltpu.SemaphoreType.DMA((devices,)),
            pltpu.SemaphoreType.DMA((devices,)),
        ]
        + step_scratch(total, frames),
        compiler_params=pltpu.CompilerParams(
            collective_id=2, has_side_effects=True, vmem_limit_bytes=40 << 20
        ),
        name="fused_step",
    )(frame_lens, label_lens, features, labels, *weights)


def sum_gradients(devices, grads):
    blocks = [grad.reshape(devices, grad.shape[0] // devices, grad.shape[1]) for grad in grads]
    shapes = [
        jax.ShapeDtypeStruct((block[0].size // LANES, LANES), jnp.float32) for block in blocks
    ]
    buffers = [pltpu.VMEM(block.shape, jnp.float32) for block in blocks]
    return pl.pallas_call(
        functools.partial(sum_kernel, devices),
        out_shape=shapes + [jax.ShapeDtypeStruct((devices, 1, LANES), jnp.float32)],
        in_specs=[VMEM] * 3,
        out_specs=[VMEM] * 4,
        scratch_shapes=buffers
        + buffers
        + [
            pltpu.VMEM((1, LANES), jnp.float32),
            pltpu.SemaphoreType.DMA((3, devices)),
            pltpu.SemaphoreType.DMA((3, devices)),
            pltpu.SemaphoreType.DMA((devices,)),
            pltpu.SemaphoreType.DMA((devices,)),
        ],
        compiler_params=pltpu.CompilerParams(
            collective_id=1, has_side_effects=True, vmem_limit_bytes=50 << 20
        ),
        name="sum_gradients",
    )(*blocks)


def adam_kernel(squares, *refs):
    weights, firsts, seconds, grads, outs = (refs[at : at + 3] for at in (0, 3, 6, 9, 12))
    new_firsts, new_seconds = refs[15:18], refs[18:21]
    total = jnp.sum(squares[...])
    clip = 1.0 / jnp.maximum(jnp.sqrt(jnp.full((1, LANES), total)), 1.0)
    for which in range(3):
        scaled = clip * grads[which][...]
        first = 0.9 * firsts[which][...] + 0.1 * scaled
        second = 0.999 * seconds[which][...] + 0.001 * scaled * scaled
        ratio = first / first_correction / (jnp.sqrt(second / second_correction) + 1e-08)
        outs[which][...] = weights[which][...] - 0.001 * ratio
        new_firsts[which][...] = first
        new_seconds[which][...] = second


def adam(squares, weights, firsts, seconds, grads):
    shapes = [jax.ShapeDtypeStruct(weight.shape, jnp.float32) for weight in weights]
    return pl.pallas_call(
        adam_kernel,
        out_shape=shapes * 3,
        in_specs=[VMEM] * 13,
        out_specs=[VMEM] * 9,
        compiler_params=pltpu.CompilerParams(vmem_limit_bytes=8 << 20),
        name="adam",
    )(squares, *weights, *firsts, *seconds, *grads)


def per_device(
    features,
    frame_lens,
    labels,
    label_lens,
    w_up,
    w_down,
    w_out,
    first_up,
    first_down,
    first_out,
    second_up,
    second_down,
    second_out,
):
    devices = lax.axis_size("dp")
    batch, frames, width = features.shape

    def lined(*arrays):
        return [array.reshape(array.shape[0] // LANES, LANES) for array in arrays]

    weights = lined(w_up, w_down, w_out)
    loss_scale = 1.0 / (batch * devices)
    rows_in = features.reshape(batch * frames, width)
    if w_up.size % (8 * FF) == 0 and w_out.size % (8 * VOCAB) == 0:
        *shares, squares = fused_step(
            loss_scale, devices, frame_lens, label_lens, rows_in, labels, weights
        )
    else:
        full_up, full_down, full_out = gather_weights(devices, *weights)
        grads = local_step(
            loss_scale,
            frame_lens,
            label_lens,
            rows_in,
            labels,
            full_up.reshape(D, FF),
            full_down.reshape(FF, D),
            full_out.reshape(D, VOCAB),
        )
        *shares, squares = sum_gradients(devices, grads)
    results = adam(
        squares,
        weights,
        lined(first_up, first_down, first_out),
        lined(second_up, second_down, second_out),
        shares,
    )
    return tuple(result.reshape(-1) for result in results)


def solution(mesh):
    flat = P("dp")
    return jax.shard_map(
        per_device,
        mesh=mesh,
        in_specs=(P("dp", None, None), flat, P("dp", None), flat) + (flat,) * 9,
        out_specs=(flat,) * 9,
        check_vma=False,
    )
```

```python
import functools

import jax
import jax.numpy as jnp
from jax import lax
from jax.experimental import pallas as pl
from jax.experimental.pallas import tpu as pltpu
from jax.sharding import PartitionSpec as P

D = 256
FF = 1024
VOCAB = 256
LANES = 128
MESH = pl.DeviceIdType.MESH

first_correction = 1.0 - (0.9**10) ** 10
second_correction = 1.0 - (0.999**10) ** 10
negative = -1e30
VMEM = pl.BlockSpec(memory_space=pltpu.VMEM)
SMEM = pl.BlockSpec(memory_space=pltpu.SMEM)
HBM = pl.BlockSpec(memory_space=pltpu.HBM)


def flip(me, bit):
    return me + bit - 2 * bit * ((me // bit) % 2)


def bit_orders(devices):
    bits = [1 << k for k in range(devices.bit_length() - 1)]
    core, rest = bits[:1], bits[1:]
    down = rest[::-1]
    swapped = down[:-2] + down[-2:][::-1]
    turned = down[-2:] + down[:-2]
    return (down + core, swapped + core, turned + core)


def subsets(bits):
    offsets = [0]
    for bit in bits:
        offsets = offsets + [offset + bit for offset in offsets]
    return offsets


def place_with(me, free, pattern):
    place = me
    for bit in free:
        if pattern & bit:
            place = flip(place, bit)
    return place


class Gather:
    def __init__(self, me, devices, fulls, send_sem, recv_sem):
        self.me, self.fulls = me, fulls
        self.send_sem, self.recv_sem = send_sem, recv_sem
        self.orders = bit_orders(devices)
        self.steps = len(self.orders[0])
        self.copies = [{}, {}, {}]

    def fill(self, shards):
        for shard, full in zip(shards, self.fulls):
            rows, width = full.shape[1:]
            parts = width // LANES
            for part in range(parts):
                full[self.me, :, part * LANES : (part + 1) * LANES] = shard[
                    pl.ds(part, rows, stride=parts), :
                ].astype(jnp.bfloat16)

    def send(self, which, pattern, stage):
        order, full = self.orders[which], self.fulls[which]
        owner = place_with(self.me, order[:stage], pattern)
        slot = pattern + order[stage]
        copy = pltpu.make_async_remote_copy(
            src_ref=full.at[owner],
            dst_ref=full.at[owner],
            send_sem=self.send_sem.at[which, slot],
            recv_sem=self.recv_sem.at[which, slot],
            device_id=(flip(self.me, order[stage]),),
            device_id_type=MESH,
        )
        copy.start()
        self.copies[which][slot] = copy

    def pass_on(self):
        for which in range(3):
            for stage in range(self.steps):
                self.send(which, 0, stage)
        for stage in range(self.steps - 1):
            for at in range(1 << stage):
                for which in range(3):
                    order = self.orders[which]
                    pattern = subsets(order[:stage])[at] + order[stage]
                    self.copies[which][pattern].wait_recv()
                    for later in range(stage + 1, self.steps):
                        self.send(which, pattern, later)

    def arrive(self, which):
        order = self.orders[which]
        for pattern in subsets(order[:-1]):
            self.copies[which][pattern + order[-1]].wait_recv()

    def close(self):
        for copies in self.copies:
            for copy in copies.values():
                copy.wait_send()


def greet(me, devices, barrier):
    @pl.loop(1, devices)
    def _(shift):
        pl.semaphore_signal(
            barrier, inc=1, device_id=((me + shift) % devices,), device_id_type=MESH
        )


def gather_kernel(devices, w_up, w_down, w_out, full_up, full_down, full_out, send_sem, recv_sem):
    me = lax.axis_index("dp")
    barrier = pltpu.get_barrier_semaphore()
    greet(me, devices, barrier)
    gather = Gather(me, devices, (full_up, full_down, full_out), send_sem, recv_sem)
    gather.fill((w_up, w_down, w_out))
    pl.semaphore_wait(barrier, devices - 1)
    gather.pass_on()
    for which in range(3):
        gather.arrive(which)
    gather.close()


def gather_weights(devices, w_up, w_down, w_out):
    shapes = []
    for shard, width in ((w_up, FF), (w_down, D), (w_out, VOCAB)):
        shapes.append(
            jax.ShapeDtypeStruct((devices, shard.size // width, width), jnp.bfloat16)
        )
    return pl.pallas_call(
        functools.partial(gather_kernel, devices),
        out_shape=shapes,
        in_specs=[VMEM] * 3,
        out_specs=[VMEM] * 3,
        scratch_shapes=[
            pltpu.SemaphoreType.DMA((3, devices)),
            pltpu.SemaphoreType.DMA((3, devices)),
        ],
        compiler_params=pltpu.CompilerParams(collective_id=0, has_side_effects=True),
        name="gather_weights",
    )(w_up, w_down, w_out)


def dot_rows(left, right):
    return jnp.dot(left, right, preferred_element_type=jnp.float32)


def dot_last(left, right, precision=None):
    return lax.dot_general(
        left, right, (((1,), (1,)), ((), ())), precision=precision,
        preferred_element_type=jnp.float32,
    )


def dot_first(left, right):
    return lax.dot_general(
        left, right, (((0,), (0,)), ((), ())), preferred_element_type=jnp.float32
    )


def row_blocks(total, body):
    block = min(128, total)

    @pl.loop(0, total // block)
    def _(step):
        body(pl.ds(pl.multiple_of(step * block, block), block))


def normalize(features, normalized):
    def body(rows):
        flat_in = features[rows, :].astype(jnp.float32)
        centre = jnp.mean(flat_in, axis=1, keepdims=True)
        shifted = flat_in - centre
        spread = jnp.mean(shifted * shifted, axis=1, keepdims=True)
        normalized[rows, :] = (shifted * lax.rsqrt(spread + 1e-05)).astype(jnp.bfloat16)

    row_blocks(features.shape[0], body)


def project_up(normalized, up_mat, activation, hidden):
    def body(rows):
        act = dot_rows(normalized[rows, :], up_mat[...].reshape(D, FF))
        activation[rows, :] = act
        hidden[rows, :] = (act * (1.0 / (1.0 + jnp.exp(-act)))).astype(jnp.bfloat16)

    row_blocks(normalized.shape[0], body)


def project_down(features, hidden, down_mat, out_mat, block_out, log_probs):
    def body(rows):
        flat_in = features[rows, :].astype(jnp.float32)
        out_rows = (flat_in + 0.5 * dot_rows(hidden[rows, :], down_mat[...].reshape(FF, D))).astype(
            jnp.bfloat16
        )
        block_out[rows, :] = out_rows
        logits = dot_rows(out_rows, out_mat[...].reshape(D, VOCAB))
        top = jnp.max(logits, axis=1, keepdims=True)
        low = logits - top
        log_probs[rows, :] = low - jnp.log(jnp.sum(jnp.exp(low), axis=1, keepdims=True))

    row_blocks(features.shape[0], body)


def ctc_grad(
    loss_scale,
    frame_lens,
    label_lens,
    labels,
    log_probs,
    emitted,
    alpha_rows,
    beta_rows,
    logit_grad,
):
    utterances, label_count = labels.shape
    frames = log_probs.shape[0] // utterances
    states = 2 * label_count + 1

    label_ids = lax.broadcasted_iota(jnp.int32, (label_count, LANES), 0)
    state_at = lax.broadcasted_iota(jnp.int32, (label_count, LANES), 1)
    spread_now = (state_at == 2 * label_ids + 1).astype(jnp.bfloat16)
    spread_back = (state_at == 2 * label_ids + 3).astype(jnp.bfloat16)
    spread_ahead = (state_at == 2 * label_ids - 1).astype(jnp.bfloat16)
    label_rows = jnp.concatenate(
        [
            labels[...].astype(jnp.float32),
            jnp.zeros((8 - utterances, label_count), jnp.float32),
        ],
        axis=0,
    ).astype(jnp.bfloat16)
    extended = dot_rows(label_rows, spread_now)
    earlier = dot_rows(label_rows, spread_back)
    later = dot_rows(label_rows, spread_ahead)
    row_ids = lax.broadcasted_iota(jnp.int32, (8, LANES), 0)
    lane_ids = lax.broadcasted_iota(jnp.int32, (8, LANES), 1)
    may_skip = (extended > 0.5) & (extended != earlier)
    skip_later = (later > 0.5) & (later != extended)
    skip_add = jnp.where(may_skip, 0.0, negative)
    later_add = jnp.where(skip_later, 0.0, negative)
    ends = jnp.full((8, LANES), -9, jnp.int32)
    first_frame = jnp.full((8, LANES), -9, jnp.int32)
    for utterance in range(utterances):
        ends = jnp.where(row_ids == utterance, 2 * label_lens[utterance], ends)
        first_frame = jnp.where(row_ids == utterance, frame_lens[utterance] - 1, first_frame)
    finish = jnp.where((lane_ids == ends) | (lane_ids == ends - 1), 0.0, negative)

    emitted[...] = jnp.full(emitted.shape, negative, jnp.float32)
    vocab_ids = lax.broadcasted_iota(jnp.int32, (VOCAB, LANES), 0).astype(jnp.float32)
    lanes_wide = lax.broadcasted_iota(jnp.int32, (VOCAB, LANES), 1)
    frame_lanes = lax.broadcasted_iota(jnp.int32, (frames, LANES), 1)
    onehots = []
    for utterance in range(utterances):
        onehot = jnp.where(
            (vocab_ids == extended[utterance : utterance + 1, :]) & (lanes_wide < states), 1.0, 0.0
        )
        onehots.append(onehot)
        picked = jnp.dot(
            log_probs[utterance * frames : (utterance + 1) * frames, :],
            onehot,
            precision=lax.Precision.HIGHEST,
            preferred_element_type=jnp.float32,
        )
        emitted[:, utterance, :] = jnp.where(frame_lanes < states, picked, negative)

    def log_three(one, two, three):
        top = jnp.maximum(jnp.maximum(one, two), three)
        return top + jnp.log(jnp.exp(one - top) + jnp.exp(two - top) + jnp.exp(three - top))

    def ahead(values, count):
        return pltpu.roll(values, count, 1) if count else values

    def behind(values, count):
        return pltpu.roll(values, LANES - count, 1) if count else values

    skips = [ahead(skip_add, count) for count in range(3)]
    later_skips = [behind(later_add, count) for count in range(3)]
    finishes = [behind(finish, count) for count in range(3)]

    def advance(pair, carry):
        alpha, weighted = carry
        frame = 2 * pair
        back = frames - 1 - frame
        moved = [ahead(alpha, count) for count in range(5)]
        other = [behind(weighted, count) for count in range(5)]
        emit, emit_back = emitted[frame], emitted[back]
        ends_here = first_frame == back
        firsts, lasts = [], []
        for count in range(3):
            base = log_three(moved[count], moved[count + 1], moved[count + 2] + skips[count])
            rest = log_three(other[count], other[count + 1], other[count + 2] + later_skips[count])
            rest = jnp.where(ends_here, finishes[count], rest)
            if count == 0:
                alpha_rows[frame] = base
                beta_rows[back] = rest
            firsts.append(base + ahead(emit, count))
            lasts.append(rest + behind(emit_back, count))
        base = log_three(firsts[0], firsts[1], firsts[2] + skips[0])
        rest = log_three(lasts[0], lasts[1], lasts[2] + later_skips[0])
        rest = jnp.where(first_frame == back - 1, finish, rest)
        alpha_rows[frame + 1] = base
        beta_rows[back - 1] = rest
        return (base + emitted[frame + 1], rest + emitted[back - 1])

    nothing = jnp.full((8, LANES), negative, jnp.float32)
    start = jnp.where(lane_ids == 0, 0.0, negative)
    lax.fori_loop(0, frames // 2, advance, (start, nothing), unroll=8)

    frame_ids = lax.broadcasted_iota(jnp.int32, (frames, LANES), 0)
    for utterance in range(utterances):
        joint = (
            alpha_rows[:, utterance, :] + emitted[:, utterance, :] + beta_rows[:, utterance, :]
        )
        top = jnp.max(joint, axis=1, keepdims=True)
        mass = jnp.exp(joint - top)
        share = mass / jnp.sum(mass, axis=1, keepdims=True)
        occupancy = jnp.where(frame_ids < frame_lens[utterance], share, 0.0)
        gamma = dot_last(occupancy, onehots[utterance], lax.Precision.HIGHEST)
        rows = slice(utterance * frames, (utterance + 1) * frames)
        probs = jnp.exp(log_probs[rows, :])
        held = jnp.sum(occupancy, axis=1, keepdims=True)
        logit_grad[rows, :] = (loss_scale * (probs * held - gamma)).astype(jnp.bfloat16)


def grad_ff(logit_grad, out_mat, ff_grad):
    def body(rows):
        ff_grad[rows, :] = (
            0.5 * dot_last(logit_grad[rows, :], out_mat[...].reshape(D, VOCAB))
        ).astype(jnp.bfloat16)

    row_blocks(logit_grad.shape[0], body)


def grad_act(ff_grad, down_mat, activation, act_grad):
    def body(rows):
        act = activation[rows, :]
        sigmoid = 1.0 / (1.0 + jnp.exp(-act))
        slope = sigmoid * (1.0 + act * (1.0 - sigmoid))
        act_grad[rows, :] = (
            dot_last(ff_grad[rows, :], down_mat[...].reshape(FF, D)) * slope
        ).astype(jnp.bfloat16)

    row_blocks(ff_grad.shape[0], body)


def step_kernel(
    loss_scale,
    frame_lens,
    label_lens,
    features,
    labels,
    up_mat,
    down_mat,
    out_mat,
    grad_up,
    grad_down,
    grad_out,
    normalized,
    activation,
    hidden,
    block_out,
    log_probs,
    emitted,
    alpha_rows,
    beta_rows,
    logit_grad,
    ff_grad,
    act_grad,
):
    normalize(features, normalized)
    project_up(normalized, up_mat, activation, hidden)
    project_down(features, hidden, down_mat, out_mat, block_out, log_probs)
    ctc_grad(
        loss_scale, frame_lens, label_lens, labels, log_probs, emitted, alpha_rows, beta_rows,
        logit_grad,
    )
    grad_ff(logit_grad, out_mat, ff_grad)
    grad_act(ff_grad, down_mat, activation, act_grad)
    grad_up[...] = dot_first(normalized[...], act_grad[...])
    grad_down[...] = dot_first(hidden[...], ff_grad[...])
    grad_out[...] = dot_first(block_out[...], logit_grad[...])


def step_scratch(total, frames):
    return [
        pltpu.VMEM((total, D), jnp.bfloat16),
        pltpu.VMEM((total, FF), jnp.float32),
        pltpu.VMEM((total, FF), jnp.bfloat16),
        pltpu.VMEM((total, D), jnp.bfloat16),
        pltpu.VMEM((total, VOCAB), jnp.float32),
        pltpu.VMEM((frames, 8, LANES), jnp.float32),
        pltpu.VMEM((frames, 8, LANES), jnp.float32),
        pltpu.VMEM((frames, 8, LANES), jnp.float32),
        pltpu.VMEM((total, VOCAB), jnp.bfloat16),
        pltpu.VMEM((total, D), jnp.bfloat16),
        pltpu.VMEM((total, FF), jnp.bfloat16),
    ]


def local_step(loss_scale, frame_lens, label_lens, features, labels, up_mat, down_mat, out_mat):
    total = features.shape[0]
    frames = total // labels.shape[0]
    return pl.pallas_call(
        functools.partial(step_kernel, loss_scale),
        out_shape=[
            jax.ShapeDtypeStruct((D, FF), jnp.float32),
            jax.ShapeDtypeStruct((FF, D), jnp.float32),
            jax.ShapeDtypeStruct((D, VOCAB), jnp.float32),
        ],
        in_specs=[SMEM, SMEM] + [VMEM] * 5,
        out_specs=[VMEM] * 3,
        scratch_shapes=step_scratch(total, frames),
        compiler_params=pltpu.CompilerParams(vmem_limit_bytes=40 << 20),
        name="local_step",
    )(frame_lens, label_lens, features, labels, up_mat, down_mat, out_mat)


class Sum:
    def __init__(self, me, devices, grads, received, staged, send_sem, recv_sem):
        self.me, self.grads, self.received, self.staged = me, grads, received, staged
        self.send_sem, self.recv_sem = send_sem, recv_sem
        self.orders = [order[::-1] for order in bit_orders(devices)]
        self.steps = len(self.orders[0])
        self.copies = [{}, {}, {}]

    def sum_of(self, which, place, pattern, stage):
        value = self.grads[which][place]
        for bit in self.orders[which][:stage]:
            self.copies[which][pattern + bit].wait_recv()
            value = value + self.received[which][pattern + bit]
        return value

    def send(self, which, stage):
        order = self.orders[which]
        for offset in subsets(order[stage + 1 :][::-1])[::-1]:
            slot = offset + order[stage]
            place = place_with(self.me, order, slot)
            if stage == 0:
                source = self.grads[which].at[place]
            else:
                self.staged[which][slot] = self.sum_of(which, place, slot, stage)
                source = self.staged[which].at[slot]
            copy = pltpu.make_async_remote_copy(
                src_ref=source,
                dst_ref=self.received[which].at[slot],
                send_sem=self.send_sem.at[which, slot],
                recv_sem=self.recv_sem.at[which, slot],
                device_id=(flip(self.me, order[stage]),),
                device_id_type=MESH,
            )
            copy.start()
            self.copies[which][slot] = copy

    def finish(self, devices, reduced, squares, own_squares, small_send, small_recv):
        me = self.me
        own = jnp.zeros((1, LANES), jnp.float32)
        for which in (2, 1, 0):
            value = self.sum_of(which, me, 0, self.steps)
            rows, width = value.shape
            parts = width // LANES
            for part in range(parts):
                piece = value[:, part * LANES : (part + 1) * LANES]
                reduced[which][pl.ds(part, rows, stride=parts), :] = piece
                own = own + jnp.sum(piece * piece, axis=0, keepdims=True)
        own_squares[...] = own
        squares[0] = own

        def small_copy(shift):
            return pltpu.make_async_remote_copy(
                src_ref=own_squares,
                dst_ref=squares.at[shift],
                send_sem=small_send.at[shift],
                recv_sem=small_recv.at[shift],
                device_id=((me + shift) % devices,),
                device_id_type=MESH,
            )

        @pl.loop(1, devices)
        def _(shift):
            small_copy(shift).start()

        for copies in self.copies:
            for copy in copies.values():
                copy.wait_send()

        @pl.loop(1, devices)
        def _(shift):
            small_copy(shift).wait()


def sum_kernel(devices, *refs):
    grads, reduced, squares = refs[:3], refs[3:6], refs[6]
    received, staged = refs[7:10], refs[10:13]
    own_squares, send_sem, recv_sem, small_send, small_recv = refs[13:]
    me = lax.axis_index("dp")
    barrier = pltpu.get_barrier_semaphore()
    greet(me, devices, barrier)
    pl.semaphore_wait(barrier, devices - 1)
    total = Sum(me, devices, grads, received, staged, send_sem, recv_sem)
    for stage in range(total.steps):
        for which in range(3):
            total.send(which, stage)
    total.finish(devices, reduced, squares, own_squares, small_send, small_recv)


def fused_kernel(devices, loss_scale, *refs):
    frame_lens, label_lens, features, labels = refs[:4]
    shards, reduced, squares = refs[4:7], refs[7:10], refs[10]
    fulls, grads, received, staged = refs[11:14], refs[14:17], refs[17:20], refs[20:23]
    gather_send, gather_recv, own_squares, send_sem, recv_sem, small_send, small_recv = refs[23:30]
    normalized, activation, hidden, block_out, log_probs = refs[30:35]
    emitted, alpha_rows, beta_rows, logit_grad, ff_grad, act_grad = refs[35:41]
    held, load_sem = refs[41:45], refs[45]
    up_mat, down_mat, out_mat = fulls
    me = lax.axis_index("dp")
    loads = [
        pltpu.make_async_copy(source, target, load_sem.at[at])
        for at, (source, target) in enumerate(zip((*shards, features), held))
    ]
    for load in loads:
        load.start()
    shards, features = held[:3], held[3]
    barrier = pltpu.get_barrier_semaphore()
    greet(me, devices, barrier)
    gather = Gather(me, devices, fulls, gather_send, gather_recv)
    for load in loads[:3]:
        load.wait()
    gather.fill(shards)
    loads[3].wait()
    normalize(features, normalized)
    pl.semaphore_wait(barrier, devices - 1)
    gather.pass_on()
    gather.arrive(0)
    project_up(normalized, up_mat, activation, hidden)
    gather.arrive(1)
    gather.arrive(2)
    project_down(features, hidden, down_mat, out_mat, block_out, log_probs)
    ctc_grad(
        loss_scale, frame_lens, label_lens, labels, log_probs, emitted, alpha_rows, beta_rows,
        logit_grad,
    )
    total = Sum(me, devices, grads, received, staged, send_sem, recv_sem)
    pending = [list(range(total.steps)) for _ in range(3)]

    def advance(*whiches):
        for which in whiches:
            if pending[which]:
                total.send(which, pending[which].pop(0))

    def put(which, value):
        grads[which][...] = value.reshape(grads[which].shape)

    grad_ff(logit_grad, out_mat, ff_grad)
    put(1, dot_first(hidden[...], ff_grad[...]))
    advance(1)
    grad_act(ff_grad, down_mat, activation, act_grad)
    advance(1)
    put(0, dot_first(normalized[...], act_grad[...]))
    advance(0)
    put(2, dot_first(block_out[...], logit_grad[...]))
    advance(2)
    while any(pending):
        advance(1, 0, 2)
    total.finish(devices, reduced, squares, own_squares, small_send, small_recv)
    gather.close()


def fused_step(loss_scale, devices, frame_lens, label_lens, features, labels, weights):
    total = features.shape[0]
    frames = total // labels.shape[0]
    blocks = [
        (devices, weight.size // width, width)
        for weight, width in zip(weights, (FF, D, VOCAB))
    ]
    wide = [pltpu.VMEM(block, jnp.float32) for block in blocks]
    return pl.pallas_call(
        functools.partial(fused_kernel, devices, loss_scale),
        out_shape=[jax.ShapeDtypeStruct(weight.shape, jnp.float32) for weight in weights]
        + [jax.ShapeDtypeStruct((devices, 1, LANES), jnp.float32)],
        in_specs=[SMEM, SMEM, HBM, VMEM] + [HBM] * 3,
        out_specs=[VMEM] * 4,
        scratch_shapes=[pltpu.VMEM(block, jnp.bfloat16) for block in blocks]
        + wide * 3
        + [
            pltpu.SemaphoreType.DMA((3, devices)),
            pltpu.SemaphoreType.DMA((3, devices)),
            pltpu.VMEM((1, LANES), jnp.float32),
            pltpu.SemaphoreType.DMA((3, devices)),
            pltpu.SemaphoreType.DMA((3, devices)),
            pltpu.SemaphoreType.DMA((devices,)),
            pltpu.SemaphoreType.DMA((devices,)),
        ]
        + step_scratch(total, frames)
        + [pltpu.VMEM(array.shape, array.dtype) for array in (*weights, features)]
        + [pltpu.SemaphoreType.DMA((4,))],
        compiler_params=pltpu.CompilerParams(
            collective_id=2, has_side_effects=True, vmem_limit_bytes=67043328
        ),
        name="fused_step",
    )(frame_lens, label_lens, features, labels, *weights)


def sum_gradients(devices, grads):
    blocks = [grad.reshape(devices, grad.shape[0] // devices, grad.shape[1]) for grad in grads]
    shapes = [
        jax.ShapeDtypeStruct((block[0].size // LANES, LANES), jnp.float32) for block in blocks
    ]
    buffers = [pltpu.VMEM(block.shape, jnp.float32) for block in blocks]
    return pl.pallas_call(
        functools.partial(sum_kernel, devices),
        out_shape=shapes + [jax.ShapeDtypeStruct((devices, 1, LANES), jnp.float32)],
        in_specs=[VMEM] * 3,
        out_specs=[VMEM] * 4,
        scratch_shapes=buffers
        + buffers
        + [
            pltpu.VMEM((1, LANES), jnp.float32),
            pltpu.SemaphoreType.DMA((3, devices)),
            pltpu.SemaphoreType.DMA((3, devices)),
            pltpu.SemaphoreType.DMA((devices,)),
            pltpu.SemaphoreType.DMA((devices,)),
        ],
        compiler_params=pltpu.CompilerParams(
            collective_id=1, has_side_effects=True, vmem_limit_bytes=50 << 20
        ),
        name="sum_gradients",
    )(*blocks)


def adam_kernel(squares, *refs):
    weights, firsts, seconds, grads, outs = (refs[at : at + 3] for at in (0, 3, 6, 9, 12))
    new_firsts, new_seconds = refs[15:18], refs[18:21]
    total = jnp.sum(squares[...])
    clip = 1.0 / jnp.maximum(jnp.sqrt(jnp.full((1, LANES), total)), 1.0)
    for which in range(3):
        scaled = clip * grads[which][...]
        first = 0.9 * firsts[which][...] + 0.1 * scaled
        second = 0.999 * seconds[which][...] + 0.001 * scaled * scaled
        ratio = first / first_correction / (jnp.sqrt(second / second_correction) + 1e-08)
        outs[which][...] = weights[which][...] - 0.001 * ratio
        new_firsts[which][...] = first
        new_seconds[which][...] = second


def adam(squares, weights, firsts, seconds, grads):
    shapes = [jax.ShapeDtypeStruct(weight.shape, jnp.float32) for weight in weights]
    return pl.pallas_call(
        adam_kernel,
        out_shape=shapes * 3,
        in_specs=[VMEM] * 13,
        out_specs=[VMEM] * 9,
        compiler_params=pltpu.CompilerParams(vmem_limit_bytes=67043328),
        name="adam",
    )(squares, *weights, *firsts, *seconds, *grads)


def per_device(
    features,
    frame_lens,
    labels,
    label_lens,
    w_up,
    w_down,
    w_out,
    first_up,
    first_down,
    first_out,
    second_up,
    second_down,
    second_out,
):
    devices = lax.axis_size("dp")
    batch, frames, width = features.shape

    def lined(*arrays):
        return [array.reshape(array.shape[0] // LANES, LANES) for array in arrays]

    weights = lined(w_up, w_down, w_out)
    loss_scale = 1.0 / (batch * devices)
    rows_in = features.reshape(batch * frames, width)
    if w_up.size % (8 * FF) == 0 and w_out.size % (8 * VOCAB) == 0:
        *shares, squares = fused_step(
            loss_scale, devices, frame_lens, label_lens, rows_in, labels, weights
        )
    else:
        full_up, full_down, full_out = gather_weights(devices, *weights)
        grads = local_step(
            loss_scale,
            frame_lens,
            label_lens,
            rows_in,
            labels,
            full_up.reshape(D, FF),
            full_down.reshape(FF, D),
            full_out.reshape(D, VOCAB),
        )
        *shares, squares = sum_gradients(devices, grads)
    results = adam(
        squares,
        weights,
        lined(first_up, first_down, first_out),
        lined(second_up, second_down, second_out),
        shares,
    )
    return tuple(result.reshape(-1) for result in results)


def solution(mesh):
    flat = P("dp")
    return jax.shard_map(
        per_device,
        mesh=mesh,
        in_specs=(P("dp", None, None), flat, P("dp", None), flat) + (flat,) * 9,
        out_specs=(flat,) * 9,
        check_vma=False,
    )
```
